32 devices in a mesh: trial: 2 (over x), shard: 4 (over y, core), cols: 4 (over z).
Axes of the slice: x: 2, y: 2, z: 4, core: 2. Of those that a mesh axis runs over, the one named last changes fastest.
Arguments:
- train_gate: bfloat16 [4096, 8192], P(('trial', 'shard'), 'cols'), parts along dimension 0, may hold values from -0.125 to 0.125
- low_gate: bfloat16 [4096, 16], P(('trial', 'shard')), parts along dimension 0, may hold values from -0.125 to 0.125
- high_gate: bfloat16 [32, 8192], P('trial', 'cols'), parts along dimension 0, may hold values from -1.5 to 1.5
- train_up: bfloat16 [4096, 8192], P(('trial', 'shard'), 'cols'), parts along dimension 0, may hold values from -0.125 to 0.125
- low_up: bfloat16 [4096, 16], P(('trial', 'shard')), parts along dimension 0, may hold values from -0.125 to 0.125
- high_up: bfloat16 [32, 8192], P('trial', 'cols'), parts along dimension 0, may hold values from -1.5 to 1.5
- norm_train: float32 [4096], P(('trial', 'shard', 'cols')), parts along dimension 0, may hold values from 0.25 to 1.75
- norm_step: float32 [4096], P(('trial', 'shard', 'cols')), parts along dimension 0, may hold values from -0.3 to 0.3
Outputs:
- serve_gate: bfloat16 [16384, 2048], P(('trial', 'cols')), parts along dimension 0
- serve_up: bfloat16 [16384, 2048], P(('trial', 'cols')), parts along dimension 0
- serve_norm: bfloat16 [4096], P('trial'), parts along dimension 0
The draws below stay inside these ranges and needn't reach their ends.
There are 2 independent parts, one for each index of `trial`. The reference program is written for one: setup_inputs(seed, part) draws one part's arguments, and reference() takes and returns one part's arrays. A program takes and returns all parts, laid end to end along the dimension named above; each array names one. Nothing has to cross between parts.
All inputs are finite; a program needn't handle non-finite values.
Results may differ from the reference program's by a relative error of at most 0.001.
Values may be sent and summed in bfloat16 or wider, within the bound.
A program may use at most 128 MiB of HBM per device.

```python
import jax
import jax.numpy as jnp

D_MODEL = 2048
D_INNER = 8192
RANK = 16


def steps_of(stream_key, extent, shards, low, largest):
    gain = 1.0
    for position, blocks in shards:
        heights = jax.random.uniform(jax.random.fold_in(jax.random.fold_in(stream_key, 6), position), (blocks,), jnp.float32, low / len(shards), largest / len(shards))
        gain = gain * jnp.repeat(jnp.exp(heights), extent[position] // blocks).reshape((-1,) + (1,) * (len(extent) - 1 - position))
    return gain


def centred(key, shape, width, reach, cuts=(), kind=jnp.bfloat16):
    loudness = steps_of(key, shape, cuts, -0.22, 0.18) if cuts else 1.0
    array = jax.random.normal(key, shape, jnp.float32) * width * loudness
    return jnp.minimum(jnp.maximum(array, -reach), reach).astype(kind)


def setup_inputs(seed: int = 0, part: int = 0) -> dict:
    key_list = jax.random.split(jax.random.key(seed), 9)
    part_splits = jax.random.split(jax.random.fold_in(key_list[8], part), 9)
    return {
        "train_gate": centred(part_splits[0], (D_MODEL, D_INNER), D_MODEL ** -0.5, 0.125, ((0, 4), (1, 4))),
        "low_gate": centred(part_splits[1], (D_MODEL, RANK), D_MODEL ** -0.5, 0.125, ((0, 4),)),
        "high_gate": centred(part_splits[2], (RANK, D_INNER), RANK ** -0.5, 1.5, ((1, 4),)),
        "train_up": centred(part_splits[3], (D_MODEL, D_INNER), D_MODEL ** -0.5, 0.125, ((0, 4), (1, 4))),
        "low_up": centred(part_splits[4], (D_MODEL, RANK), D_MODEL ** -0.5, 0.125, ((0, 4),)),
        "high_up": centred(part_splits[5], (RANK, D_INNER), RANK ** -0.5, 1.5, ((1, 4),)),
        "norm_train": jnp.clip(1.0 + 0.15 * jax.random.normal(part_splits[6], (D_MODEL,), jnp.float32), 0.25, 1.75),
        "norm_step": jnp.clip(jax.random.uniform(part_splits[7], (D_MODEL,), jnp.float32, -0.3, 0.3) * steps_of(part_splits[7], (D_MODEL,), ((0, 16),), -0.4, 0.0), -0.3, 0.3),
    }


mix_rate = 2.0


def reference(train_gate, low_gate, high_gate, train_up, low_up, high_up, norm_train, norm_step):
    fresh_gate = train_gate.astype(jnp.float32) + mix_rate * jnp.dot(low_gate, high_gate, preferred_element_type=jnp.float32)
    fresh_up = train_up.astype(jnp.float32) + mix_rate * jnp.dot(low_up, high_up, preferred_element_type=jnp.float32)
    serve_gate = fresh_gate.T.astype(jnp.bfloat16)
    serve_up = fresh_up.T.astype(jnp.bfloat16)
    serve_norm = (norm_train + norm_step).astype(jnp.bfloat16)
    return serve_gate, serve_up, serve_norm
```

```python
import functools

import jax
import jax.numpy as jnp
from jax import lax
from jax.experimental import pallas as pl
from jax.experimental.pallas import tpu as pltpu
from jax.sharding import PartitionSpec as P


mix_rate = 2.0
ANY = pl.BlockSpec(memory_space=pl.ANY)
TILE = 256
PIECES = ((1, 2, 2, 3), (3, 2, 2, 1))
UNITS = 8


def merge_kernel(train_ref, low_ref, high_ref, out_ref):
    change = lax.dot_general(
        low_ref[...],
        high_ref[...],
        (((0,), (0,)), ((), ())),
        preferred_element_type=jnp.float32,
    )
    fresh = train_ref[...].astype(jnp.float32) + mix_rate * change
    out_ref[...] = fresh.astype(jnp.bfloat16).T


def merge(train, low, high, first, size):
    rank, rows = low.shape
    tile = TILE
    skip = first // tile
    return pl.pallas_call(
        merge_kernel,
        grid=(size // tile,),
        in_specs=[
            pl.BlockSpec((rows, tile), lambda i: (0, i + skip)),
            pl.BlockSpec((rank, rows), lambda i: (0, 0)),
            pl.BlockSpec((rank, tile), lambda i: (0, i + skip)),
        ],
        out_specs=pl.BlockSpec((tile, rows), lambda i: (i, 0)),
        out_shape=jax.ShapeDtypeStruct((size, rows), jnp.bfloat16),
        cost_estimate=pl.CostEstimate(
            flops=2 * size * rows * rank, bytes_accessed=4 * size * rows, transcendentals=0
        ),
    )(train, low, high)


def place_kernel(masks, first, started, *refs):
    blocks = refs[: len(masks)]
    out_ref, held, in_sem, out_sem = refs[len(masks) + (1 if started else 0) :]
    size, width = blocks[0].shape
    me = lax.axis_index("shard")
    loads, stores = [], []
    for j, block in enumerate(blocks):
        load = pltpu.make_async_copy(block, held.at[j], in_sem.at[j])
        load.start()
        loads.append(load)
    for j, mask in enumerate(masks):
        loads[j].wait()
        column = pl.multiple_of((me ^ mask) * width, width)
        store = pltpu.make_async_copy(
            held.at[j],
            out_ref.at[pl.ds(first, size), pl.ds(column, width)],
            out_sem.at[j],
        )
        store.start()
        stores.append(store)
    for store in stores:
        store.wait()


def place(whole, shape, blocks, masks, first):
    started = whole is not None
    count = len(blocks)
    return pl.pallas_call(
        functools.partial(place_kernel, masks, first, started),
        in_specs=[ANY] * (count + started),
        out_specs=ANY,
        out_shape=jax.ShapeDtypeStruct(shape, jnp.bfloat16),
        scratch_shapes=[
            pltpu.VMEM((count,) + blocks[0].shape, jnp.bfloat16),
            pltpu.SemaphoreType.DMA((count,)),
            pltpu.SemaphoreType.DMA((count,)),
        ],
        input_output_aliases={count: 0} if started else {},
        cost_estimate=pl.CostEstimate(
            flops=0, bytes_accessed=4 * count * blocks[0].size, transcendentals=0
        ),
    )(*blocks, *([whole] if started else []))


def swap(x, axis, size, bit):
    return lax.ppermute(x, axis, [(i, i ^ bit) for i in range(size)])


def cuts(inner):
    found = []
    for which, units in enumerate(PIECES):
        first = 0
        for unit in units:
            found.append((which, first, unit * inner // UNITS))
            first += found[-1][2]
    return found


def gathered(n, pairs):
    rows, inner = pairs[0][0].shape
    queue = []
    for which, first, size in cuts(inner):
        train, low, high = pairs[which]
        own = merge(train, low.T, high, first, size)
        queue.append((which, first, [own, swap(own, "shard", n, n // 2)], [0, n // 2]))
    whole, last = [None] * len(pairs), None
    for which, first, held, masks in queue:
        if last is not None:
            whole[last], held[1] = lax.optimization_barrier((whole[last], held[1]))
        bit = n // 4
        while bit:
            held = held + [swap(h, "shard", n, bit) for h in held]
            masks = masks + [m ^ bit for m in masks]
            bit //= 2
        whole[which] = place(whole[which], (inner, n * rows), held, tuple(masks), first)
        last = which
    return whole


def norm_gathered(n, m, gain):
    me = lax.axis_index("shard") * m + lax.axis_index("cols")
    held = jnp.where(jnp.arange(n * m)[:, None] == me, gain[None, :], jnp.zeros((), gain.dtype))
    for axis, size in (("cols", m), ("shard", n)):
        bit = 1
        while bit < size:
            held = held + swap(held, axis, size, bit)
            bit *= 2
    return held.reshape(-1)


def plain(train, low, high):
    fresh = train.astype(jnp.float32) + mix_rate * jnp.dot(
        low, high, preferred_element_type=jnp.float32
    )
    return lax.all_gather(fresh.astype(jnp.bfloat16), "shard", axis=0, tiled=True).T


def power(n):
    return n & (n - 1) == 0


def fits(n, m, rows, inner):
    return n > 1 and power(n) and power(m) and rows % 128 == 0 and inner % (TILE * UNITS) == 0


def local(n, m, train_gate, low_gate, high_gate, train_up, low_up, high_up, norm_train, norm_step):
    pairs = [(train_gate, low_gate, high_gate), (train_up, low_up, high_up)]
    gain = (norm_train + norm_step).astype(jnp.bfloat16)
    if not fits(n, m, *train_gate.shape):
        serve_gate, serve_up = [plain(*pair) for pair in pairs]
        serve_norm = lax.all_gather(gain, ("shard", "cols"), axis=0, tiled=True)
        return serve_gate, serve_up, serve_norm
    serve_norm = norm_gathered(n, m, gain)
    serve_gate, serve_up = gathered(n, pairs)
    return serve_gate, serve_up, serve_norm


def solution(mesh):
    n, m = mesh.shape["shard"], mesh.shape["cols"]
    return jax.shard_map(
        functools.partial(local, n, m),
        mesh=mesh,
        in_specs=(
            P(("trial", "shard"), "cols"),
            P(("trial", "shard"), None),
            P("trial", "cols"),
            P(("trial", "shard"), "cols"),
            P(("trial", "shard"), None),
            P("trial", "cols"),
            P(("trial", "shard", "cols")),
            P(("trial", "shard", "cols")),
        ),
        out_specs=(P(("trial", "cols"), None), P(("trial", "cols"), None), P("trial")),
        check_vma=False,
    )
```

```python
import functools

import jax
import jax.numpy as jnp
from jax import lax
from jax.experimental import pallas as pl
from jax.experimental.pallas import tpu as pltpu
from jax.sharding import PartitionSpec as P


mix_rate = 2.0
ANY = pl.BlockSpec(memory_space=pl.ANY)
RAW_PARTS = 2
PIECES = (6, 4, 2, 2, 1, 1)
UNITS = sum(PIECES)
GRANT = pltpu.CompilerParams(vmem_limit_bytes=12 * 2**20)


def merge_kernel(train_ref, low_ref, high_ref, out_ref):
    change = lax.dot_general(
        low_ref[...],
        high_ref[...],
        (((0,), (0,)), ((), ())),
        preferred_element_type=jnp.float32,
    )
    fresh = train_ref[...].astype(jnp.float32) + mix_rate * change
    out_ref[...] = fresh.astype(jnp.bfloat16).T


def merge(train, low, high, first, size):
    rank, rows = low.shape
    tile = 256 if first % 256 == 0 and size % 256 == 0 else 128
    skip = first // tile
    return pl.pallas_call(
        merge_kernel,
        grid=(size // tile,),
        in_specs=[
            pl.BlockSpec((rows, tile), lambda i: (0, i + skip)),
            pl.BlockSpec((rank, rows), lambda i: (0, 0)),
            pl.BlockSpec((rank, tile), lambda i: (0, i + skip)),
        ],
        out_specs=pl.BlockSpec((tile, rows), lambda i: (i, 0)),
        out_shape=jax.ShapeDtypeStruct((size, rows), jnp.bfloat16),
        compiler_params=GRANT,
        cost_estimate=pl.CostEstimate(
            flops=2 * size * rows * rank, bytes_accessed=4 * size * rows, transcendentals=0
        ),
    )(train, low, high)


def place_kernel(spots, started, *refs):
    count = len(spots)
    blocks = refs[:count]
    out_ref = refs[count + started]
    held = refs[count + started + 1 : -2]
    in_sem, out_sem = refs[-2:]
    me = lax.axis_index("shard")
    loads, stores = [], []
    for j, block in enumerate(blocks):
        load = pltpu.make_async_copy(block, held[j], in_sem.at[j])
        load.start()
        loads.append(load)
    for j, (mask, first) in enumerate(spots):
        loads[j].wait()
        size, width = blocks[j].shape
        column = pl.multiple_of((me ^ mask) * width, width)
        store = pltpu.make_async_copy(
            held[j], out_ref.at[pl.ds(first, size), pl.ds(column, width)], out_sem.at[j]
        )
        store.start()
        stores.append(store)
    for store in stores:
        store.wait()


def place(whole, shape, blocks, spots):
    started = whole is not None
    count = len(blocks)
    return pl.pallas_call(
        functools.partial(place_kernel, spots, started),
        in_specs=[ANY] * (count + started),
        out_specs=ANY,
        out_shape=jax.ShapeDtypeStruct(shape, jnp.bfloat16),
        scratch_shapes=[
            *[pltpu.VMEM(block.shape, jnp.bfloat16) for block in blocks],
            pltpu.SemaphoreType.DMA((count,)),
            pltpu.SemaphoreType.DMA((count,)),
        ],
        input_output_aliases={count: 0} if started else {},
        compiler_params=GRANT,
        cost_estimate=pl.CostEstimate(
            flops=0, bytes_accessed=4 * sum(b.size for b in blocks), transcendentals=0
        ),
    )(*blocks, *([whole] if started else []))


def swap(x, axis, size, bit):
    return lax.ppermute(x, axis, [(i, i ^ bit) for i in range(size)])


def near(n, held, masks):
    held, masks = [held], [masks]
    bit = n // 4
    while bit:
        held = held + [swap(h, "shard", n, bit) for h in held]
        masks = masks + [m ^ bit for m in masks]
        bit //= 2
    return held, masks


def gathered(n, gate, up):
    train_gate, low_gate, high_gate = gate
    train_up, low_up, high_up = up
    rows, inner = train_gate.shape
    shape = (inner, n * rows)
    far = n // 2
    raw = swap(train_gate, "shard", n, far)
    raw_low = swap(low_gate.T, "shard", n, far)

    pieces, first = [], 0
    for unit in PIECES:
        size = unit * inner // UNITS
        own = merge(train_up, low_up.T, high_up, first, size)
        pieces.append((first, size, own, swap(own, "shard", n, far)))
        first += size
    held, masks = near(n, merge(train_gate, low_gate.T, high_gate, 0, inner), 0)
    whole_gate = place(None, shape, held, tuple((m, 0) for m in masks))
    blocks, spots = [], []
    for first, size, own, _ in pieces:
        held, masks = near(n, own, 0)
        blocks += held
        spots += [(m, first) for m in masks]
    whole_up = place(None, shape, blocks, tuple(spots))

    raw, whole_gate, whole_up = lax.optimization_barrier((raw, whole_gate, whole_up))
    size = inner // RAW_PARTS
    for first in range(0, inner, size):
        part = merge(raw, raw_low, high_gate, first, size)
        held, masks = near(n, part, far)
        whole_gate = place(whole_gate, shape, held, tuple((m, first) for m in masks))
    for k, (first, size, _, part) in enumerate(pieces):
        if k:
            part, whole_up = lax.optimization_barrier((part, whole_up))
        else:
            part, whole_up, whole_gate = lax.optimization_barrier((part, whole_up, whole_gate))
        held, masks = near(n, part, far)
        whole_up = place(whole_up, shape, held, tuple((m, first) for m in masks))
    return whole_gate, whole_up


def norm_gathered(n, m, gain):
    me = lax.axis_index("shard") * m + lax.axis_index("cols")
    held = jnp.where(jnp.arange(n * m)[:, None] == me, gain[None, :], jnp.zeros((), gain.dtype))
    for axis, size in (("cols", m), ("shard", n)):
        bit = 1
        while bit < size:
            held = held + swap(held, axis, size, bit)
            bit *= 2
    return held.reshape(-1)


def plain(train, low, high):
    fresh = train.astype(jnp.float32) + mix_rate * jnp.dot(
        low, high, preferred_element_type=jnp.float32
    )
    return lax.all_gather(fresh.astype(jnp.bfloat16), "shard", axis=0, tiled=True).T


def power(n):
    return n & (n - 1) == 0


def fits(n, m, rows, inner):
    return n > 1 and power(n) and power(m) and rows % 128 == 0 and inner % (128 * UNITS) == 0


def local(n, m, train_gate, low_gate, high_gate, train_up, low_up, high_up, norm_train, norm_step):
    pairs = [(train_gate, low_gate, high_gate), (train_up, low_up, high_up)]
    gain = (norm_train + norm_step).astype(jnp.bfloat16)
    if not fits(n, m, *train_gate.shape):
        serve_gate, serve_up = [plain(*pair) for pair in pairs]
        serve_norm = lax.all_gather(gain, ("shard", "cols"), axis=0, tiled=True)
        return serve_gate, serve_up, serve_norm
    serve_norm = norm_gathered(n, m, gain)
    serve_gate, serve_up = gathered(n, *pairs)
    return serve_gate, serve_up, serve_norm


def solution(mesh):
    n, m = mesh.shape["shard"], mesh.shape["cols"]
    return jax.shard_map(
        functools.partial(local, n, m),
        mesh=mesh,
        in_specs=(
            P(("trial", "shard"), "cols"),
            P(("trial", "shard"), None),
            P("trial", "cols"),
            P(("trial", "shard"), "cols"),
            P(("trial", "shard"), None),
            P("trial", "cols"),
            P(("trial", "shard", "cols")),
            P(("trial", "shard", "cols")),
        ),
        out_specs=(P(("trial", "cols"), None), P(("trial", "cols"), None), P("trial")),
        check_vma=False,
    )
```

```python
import functools

import jax
import jax.numpy as jnp
from jax import lax
from jax.experimental import pallas as pl
from jax.experimental.pallas import tpu as pltpu
from jax.sharding import PartitionSpec as P


mix_rate = 2.0
ANY = pl.BlockSpec(memory_space=pl.ANY)
RAW_PARTS = 2
PIECES = (6, 4, 3, 2, 1)
UNITS = sum(PIECES)
GRANT = pltpu.CompilerParams(vmem_limit_bytes=12 * 2**20)


def merge_kernel(train_ref, low_ref, high_ref, out_ref):
    change = lax.dot_general(
        low_ref[...],
        high_ref[...],
        (((0,), (0,)), ((), ())),
        preferred_element_type=jnp.float32,
    )
    fresh = train_ref[...].astype(jnp.float32) + mix_rate * change
    out_ref[...] = fresh.astype(jnp.bfloat16).T


def merge(train, low, high, first, size):
    rank, rows = low.shape
    tile = 256 if first % 256 == 0 and size % 256 == 0 else 128
    skip = first // tile
    return pl.pallas_call(
        merge_kernel,
        grid=(size // tile,),
        in_specs=[
            pl.BlockSpec((rows, tile), lambda i: (0, i + skip)),
            pl.BlockSpec((rank, rows), lambda i: (0, 0)),
            pl.BlockSpec((rank, tile), lambda i: (0, i + skip)),
        ],
        out_specs=pl.BlockSpec((tile, rows), lambda i: (i, 0)),
        out_shape=jax.ShapeDtypeStruct((size, rows), jnp.bfloat16),
        compiler_params=GRANT,
        cost_estimate=pl.CostEstimate(
            flops=2 * size * rows * rank, bytes_accessed=4 * size * rows, transcendentals=0
        ),
    )(train, low, high)


def place_kernel(spots, *refs):
    count = len(spots)
    blocks = refs[:count]
    out_ref = refs[count]
    held = refs[count + 1 : -2]
    in_sem, out_sem = refs[-2:]
    me = lax.axis_index("shard")
    loads, stores = [], []
    for j, block in enumerate(blocks):
        load = pltpu.make_async_copy(block, held[j], in_sem.at[j])
        load.start()
        loads.append(load)
    for j, (mask, first) in enumerate(spots):
        loads[j].wait()
        size, width = blocks[j].shape
        column = pl.multiple_of((me ^ mask) * width, width)
        store = pltpu.make_async_copy(
            held[j], out_ref.at[pl.ds(first, size), pl.ds(column, width)], out_sem.at[j]
        )
        store.start()
        stores.append(store)
    for store in stores:
        store.wait()


def land_kernel(spots, *refs):
    out_ref, sem = refs[-2:]
    me = lax.axis_index("shard")
    stores = []
    for j, (mask, first) in enumerate(spots):
        size, width = refs[j].shape
        column = pl.multiple_of((me ^ mask) * width, width)
        store = pltpu.make_async_copy(
            refs[j], out_ref.at[pl.ds(first, size), pl.ds(column, width)], sem.at[j]
        )
        store.start()
        stores.append(store)
    for store in stores:
        store.wait()


def land(whole, blocks, spots):
    count = len(blocks)
    return pl.pallas_call(
        functools.partial(land_kernel, spots),
        in_specs=[ANY] * (count + 1),
        out_specs=ANY,
        out_shape=jax.ShapeDtypeStruct(whole.shape, whole.dtype),
        scratch_shapes=[pltpu.SemaphoreType.DMA((count,))],
        input_output_aliases={count: 0},
        compiler_params=GRANT,
        cost_estimate=pl.CostEstimate(
            flops=0, bytes_accessed=4 * sum(b.size for b in blocks), transcendentals=0
        ),
    )(*blocks, whole)


def place(shape, blocks, spots):
    count = len(blocks)
    return pl.pallas_call(
        functools.partial(place_kernel, spots),
        in_specs=[ANY] * count,
        out_specs=ANY,
        out_shape=jax.ShapeDtypeStruct(shape, jnp.bfloat16),
        scratch_shapes=[
            *[pltpu.VMEM(block.shape, jnp.bfloat16) for block in blocks],
            pltpu.SemaphoreType.DMA((count,)),
            pltpu.SemaphoreType.DMA((count,)),
        ],
        compiler_params=GRANT,
        cost_estimate=pl.CostEstimate(
            flops=0, bytes_accessed=4 * sum(b.size for b in blocks), transcendentals=0
        ),
    )(*blocks)


def swap(x, axis, size, bit):
    return lax.ppermute(x, axis, [(i, i ^ bit) for i in range(size)])


def near(n, held, masks):
    held, masks = [held], [masks]
    bit = n // 4
    while bit:
        held = held + [swap(h, "shard", n, bit) for h in held]
        masks = masks + [m ^ bit for m in masks]
        bit //= 2
    return held, masks


def gathered(n, gate, up):
    train_gate, low_gate, high_gate = gate
    train_up, low_up, high_up = up
    rows, inner = train_gate.shape
    shape = (inner, n * rows)
    far = n // 2
    raw = swap(train_gate, "shard", n, far)
    raw_low = swap(low_gate.T, "shard", n, far)

    pieces, first = [], 0
    for unit in PIECES:
        size = unit * inner // UNITS
        own = merge(train_up, low_up.T, high_up, first, size)
        pieces.append((first, size, own, swap(own, "shard", n, far)))
        first += size
    held, masks = near(n, merge(train_gate, low_gate.T, high_gate, 0, inner), 0)
    whole_gate = place(shape, held, tuple((m, 0) for m in masks))
    blocks, spots = [], []
    for first, size, own, _ in pieces:
        held, masks = near(n, own, 0)
        blocks += held
        spots += [(m, first) for m in masks]
    whole_up = place(shape, blocks, tuple(spots))

    raw, whole_gate, whole_up = lax.optimization_barrier((raw, whole_gate, whole_up))
    size = inner // RAW_PARTS
    for first in range(0, inner, size):
        part = merge(raw, raw_low, high_gate, first, size)
        held, masks = near(n, part, far)
        whole_gate = land(whole_gate, held, tuple((m, first) for m in masks))
    for k, (first, size, _, part) in enumerate(pieces):
        if k:
            part, whole_up = lax.optimization_barrier((part, whole_up))
        else:
            part, whole_up, whole_gate = lax.optimization_barrier((part, whole_up, whole_gate))
        held, masks = near(n, part, far)
        whole_up = land(whole_up, held, tuple((m, first) for m in masks))
    return whole_gate, whole_up


def norm_gathered(n, m, gain):
    me = lax.axis_index("shard") * m + lax.axis_index("cols")
    held = jnp.where(jnp.arange(n * m)[:, None] == me, gain[None, :], jnp.zeros((), gain.dtype))
    for axis, size in (("cols", m), ("shard", n)):
        bit = 1
        while bit < size:
            held = held + swap(held, axis, size, bit)
            bit *= 2
    return held.reshape(-1)


def plain(train, low, high):
    fresh = train.astype(jnp.float32) + mix_rate * jnp.dot(
        low, high, preferred_element_type=jnp.float32
    )
    return lax.all_gather(fresh.astype(jnp.bfloat16), "shard", axis=0, tiled=True).T


def power(n):
    return n & (n - 1) == 0


def fits(n, m, rows, inner):
    return n > 1 and power(n) and power(m) and rows % 128 == 0 and inner % (128 * UNITS) == 0


def local(n, m, train_gate, low_gate, high_gate, train_up, low_up, high_up, norm_train, norm_step):
    pairs = [(train_gate, low_gate, high_gate), (train_up, low_up, high_up)]
    gain = (norm_train + norm_step).astype(jnp.bfloat16)
    if not fits(n, m, *train_gate.shape):
        serve_gate, serve_up = [plain(*pair) for pair in pairs]
        serve_norm = lax.all_gather(gain, ("shard", "cols"), axis=0, tiled=True)
        return serve_gate, serve_up, serve_norm
    serve_norm = norm_gathered(n, m, gain)
    serve_gate, serve_up = gathered(n, *pairs)
    return serve_gate, serve_up, serve_norm


def solution(mesh):
    n, m = mesh.shape["shard"], mesh.shape["cols"]
    return jax.shard_map(
        functools.partial(local, n, m),
        mesh=mesh,
        in_specs=(
            P(("trial", "shard"), "cols"),
            P(("trial", "shard"), None),
            P("trial", "cols"),
            P(("trial", "shard"), "cols"),
            P(("trial", "shard"), None),
            P("trial", "cols"),
            P(("trial", "shard", "cols")),
            P(("trial", "shard", "cols")),
        ),
        out_specs=(P(("trial", "cols"), None), P(("trial", "cols"), None), P("trial")),
        check_vma=False,
    )
```
